8 devices in a mesh: tp: 8 (over z, y, x, core).
Axes of the slice: x: 2, y: 2, z: 1, core: 2. Of those that a mesh axis runs over, the one named last changes fastest.
Arguments:
- hidden_in: bfloat16 [12, 768, 4096], P(None, 'tp')
- lengths: int32 [12], replicated
- attn_norm: bfloat16 [2, 4096], replicated
- w_query: bfloat16 [2, 4096, 32, 128], replicated
- w_key: bfloat16 [2, 4096, 8, 128], replicated
- w_value: bfloat16 [2, 4096, 8, 128], replicated
- w_out: bfloat16 [2, 32, 128, 4096], replicated
- mlp_norm: bfloat16 [2, 4096], replicated
- w_gate: bfloat16 [2, 4096, 14336], P(None, None, 'tp')
- w_up: bfloat16 [2, 4096, 14336], P(None, None, 'tp')
- w_down: bfloat16 [2, 14336, 4096], P(None, 'tp')
- final_norm: bfloat16 [4096], replicated
Outputs:
- output: bfloat16 [12, 768, 4096], P(None, 'tp')
All inputs are finite; a program needn't handle non-finite values.
Results may differ from the reference program's by a relative error of at most 0.02.
Values are sent between devices in bfloat16 or wider.
A program may use at most 1.25 GiB of HBM per device.

```python
import jax
import jax.numpy as jnp
from jax import lax

BATCH = 12
SEQ_DEV = 96
TP_SIZE = 8
SEQ_LEN = 768
D_MODEL = 4096
HEADS = 32
KV_HEADS = 8
HEAD_DIM = 128
FF_DIM = 14336
LAYERS = 2

NORM_EPS = 1e-5
ROPE_BASE = 500000.0


def setup_inputs(seed: int = 0) -> dict:
    keys = jax.random.split(jax.random.key(seed), 12)
    d_scale = D_MODEL ** -0.5
    hidden_in = jax.random.normal(keys[0], (BATCH, SEQ_LEN, D_MODEL), jnp.float32)
    lengths = jax.random.randint(keys[1], (BATCH,), 1, SEQ_LEN + 1, jnp.int32)
    attn_norm = 1.0 + 0.25 * jax.random.normal(keys[2], (LAYERS, D_MODEL), jnp.float32)
    w_query = 1.4 * d_scale * jax.random.normal(keys[3], (LAYERS, D_MODEL, HEADS, HEAD_DIM), jnp.float32)
    w_key = 1.4 * d_scale * jax.random.normal(keys[4], (LAYERS, D_MODEL, KV_HEADS, HEAD_DIM), jnp.float32)
    w_value = d_scale * jax.random.normal(keys[5], (LAYERS, D_MODEL, KV_HEADS, HEAD_DIM), jnp.float32)
    w_out = (HEADS * HEAD_DIM) ** -0.5 * jax.random.normal(keys[6], (LAYERS, HEADS, HEAD_DIM, D_MODEL), jnp.float32)
    mlp_norm = 1.0 + 0.25 * jax.random.normal(keys[7], (LAYERS, D_MODEL), jnp.float32)
    w_gate = d_scale * jax.random.normal(keys[8], (LAYERS, D_MODEL, FF_DIM), jnp.float32)
    w_up = d_scale * jax.random.normal(keys[9], (LAYERS, D_MODEL, FF_DIM), jnp.float32)
    w_down = FF_DIM ** -0.5 * jax.random.normal(keys[10], (LAYERS, FF_DIM, D_MODEL), jnp.float32)
    final_norm = 1.0 + 0.25 * jax.random.normal(keys[11], (D_MODEL,), jnp.float32)
    return {
        'hidden_in': hidden_in.astype(jnp.bfloat16),
        'lengths': lengths,
        'attn_norm': attn_norm.astype(jnp.bfloat16),
        'w_query': w_query.astype(jnp.bfloat16),
        'w_key': w_key.astype(jnp.bfloat16),
        'w_value': w_value.astype(jnp.bfloat16),
        'w_out': w_out.astype(jnp.bfloat16),
        'mlp_norm': mlp_norm.astype(jnp.bfloat16),
        'w_gate': w_gate.astype(jnp.bfloat16),
        'w_up': w_up.astype(jnp.bfloat16),
        'w_down': w_down.astype(jnp.bfloat16),
        'final_norm': final_norm.astype(jnp.bfloat16),
    }


def rms_norm(hidden, gain):
    h_wide = hidden.astype(jnp.float32)
    inv_rms = lax.rsqrt(jnp.mean(h_wide * h_wide, axis=-1, keepdims=True) + NORM_EPS)
    return (h_wide * inv_rms * gain.astype(jnp.float32)).astype(jnp.bfloat16)


def rotate(proj, cos_tab, sin_tab):
    half_dim = proj.shape[-1] // 2
    first = proj[..., :half_dim]
    second = proj[..., half_dim:]
    return jnp.concatenate([first * cos_tab - second * sin_tab, second * cos_tab + first * sin_tab], axis=-1)


def reference(hidden_in, lengths, attn_norm, w_query, w_key, w_value, w_out, mlp_norm, w_gate, w_up, w_down, final_norm):
    groups = HEADS // KV_HEADS
    ff_shard = FF_DIM // TP_SIZE
    half_dim = HEAD_DIM // 2
    positions = jnp.arange(SEQ_LEN)
    inv_freq = ROPE_BASE ** (-2.0 * jnp.arange(half_dim).astype(jnp.float32) / HEAD_DIM)
    angles = positions.astype(jnp.float32)[:, None, None] * inv_freq[None, None, :]
    cos_tab = jnp.cos(angles)
    sin_tab = jnp.sin(angles)
    score_scale = HEAD_DIM ** -0.5
    key_ok = positions[None, :] < lengths[:, None]

    def layer_fn(hidden, layer_w):
        g_attn, w_q, w_k, w_v, w_o, g_mlp, w_g, w_u, w_d = layer_w
        normed = rms_norm(hidden, g_attn).astype(jnp.float32)
        q_proj = jnp.einsum('bsd,dhe->bshe', normed, w_q.astype(jnp.float32))
        key_proj = jnp.einsum('bsd,dhe->bshe', normed, w_k.astype(jnp.float32))
        v_proj = jnp.einsum('bsd,dhe->bshe', normed, w_v.astype(jnp.float32)).astype(jnp.bfloat16)
        q_rot = rotate(q_proj, cos_tab, sin_tab).astype(jnp.bfloat16)
        k_rot = rotate(key_proj, cos_tab, sin_tab).astype(jnp.bfloat16)
        q_blocks = jnp.moveaxis(q_rot.reshape(BATCH, TP_SIZE, SEQ_DEV, KV_HEADS, groups, HEAD_DIM), 1, 0)
        k_wide = k_rot.astype(jnp.float32)
        v_wide = v_proj.astype(jnp.float32)

        def block_fn(blk_args):
            q_blk, blk_idx = blk_args
            q_pos = blk_idx * SEQ_DEV + jnp.arange(SEQ_DEV)
            scores = jnp.einsum('bqkgd,bskd->bkgqs', q_blk.astype(jnp.float32), k_wide) * score_scale
            allowed = (positions[None, None, :] <= q_pos[None, :, None]) & key_ok[:, None, :]
            scores = jnp.where(allowed[:, None, None, :, :], scores, -1e30)
            prob_mat = jax.nn.softmax(scores, axis=-1).astype(jnp.bfloat16)
            context = jnp.einsum('bkgqs,bskd->bqkgd', prob_mat.astype(jnp.float32), v_wide)
            return context.astype(jnp.bfloat16)

        context = lax.map(block_fn, (q_blocks, jnp.arange(TP_SIZE)))
        context = jnp.moveaxis(context, 0, 1).reshape(BATCH, SEQ_LEN, HEADS, HEAD_DIM)
        attn_out = jnp.einsum('bshe,hed->bsd', context.astype(jnp.float32), w_o.astype(jnp.float32))
        hidden = (hidden.astype(jnp.float32) + attn_out).astype(jnp.bfloat16)
        normed = rms_norm(hidden, g_mlp).reshape(BATCH * SEQ_LEN, D_MODEL)
        wg_shards = jnp.moveaxis(w_g.reshape(D_MODEL, TP_SIZE, ff_shard), 1, 0)
        wu_shards = jnp.moveaxis(w_u.reshape(D_MODEL, TP_SIZE, ff_shard), 1, 0)
        wd_shards = w_d.reshape(TP_SIZE, ff_shard, D_MODEL)

        def shard_fn(acc_sum, shard_w):
            g_w, u_w, d_w = shard_w
            gate_proj = jnp.dot(normed, g_w, preferred_element_type=jnp.float32)
            up_proj = jnp.dot(normed, u_w, preferred_element_type=jnp.float32)
            gated_act = (jax.nn.silu(gate_proj) * up_proj).astype(jnp.bfloat16)
            part_out = jnp.dot(gated_act, d_w, preferred_element_type=jnp.float32).astype(jnp.bfloat16)
            return acc_sum + part_out.astype(jnp.float32), None

        mlp_out, unused = lax.scan(shard_fn, jnp.zeros((BATCH * SEQ_LEN, D_MODEL), jnp.float32), (wg_shards, wu_shards, wd_shards))
        hidden = (hidden.astype(jnp.float32) + mlp_out.reshape(BATCH, SEQ_LEN, D_MODEL)).astype(jnp.bfloat16)
        return hidden, None

    hidden, unused = lax.scan(layer_fn, hidden_in, (attn_norm, w_query, w_key, w_value, w_out, mlp_norm, w_gate, w_up, w_down))
    return rms_norm(hidden, final_norm)
```

```python
import functools

import jax
import jax.numpy as jnp
from jax import lax
from jax.experimental import pallas as pl
from jax.experimental.pallas import tpu as pltpu
from jax.sharding import PartitionSpec as P

NORM_EPS = 1e-5
ROPE_BASE = 500000.0


def rms_norm(hidden, gain):
    h_wide = hidden.astype(jnp.float32)
    inv_rms = lax.rsqrt(jnp.mean(h_wide * h_wide, axis=-1, keepdims=True) + NORM_EPS)
    return (h_wide * inv_rms * gain.astype(jnp.float32)).astype(jnp.bfloat16)


def rope_tables(positions, head_dim):
    half_dim = head_dim // 2
    inv_freq = ROPE_BASE ** (-2.0 * jnp.arange(half_dim).astype(jnp.float32) / head_dim)
    angles = positions.astype(jnp.float32)[:, None, None] * inv_freq[None, None, :]
    return jnp.cos(angles), jnp.sin(angles)


def rotate(proj, cos_tab, sin_tab):
    half_dim = proj.shape[-1] // 2
    first = proj[..., :half_dim]
    second = proj[..., half_dim:]
    return jnp.concatenate([first * cos_tab - second * sin_tab, second * cos_tab + first * sin_tab], axis=-1)


def norm_kernel(h_ref, gain_ref, z_ref):
    z_ref[0] = rms_norm(h_ref[0], gain_ref[...])


def norm_rows(blocks, gain, major):
    n, rows, width = blocks.shape
    minor = n // major
    return pl.pallas_call(
        norm_kernel,
        grid=(n,),
        in_specs=[
            pl.BlockSpec((1, rows, width), lambda i: ((i % minor) * major + i // minor, 0, 0)),
            pl.BlockSpec((1, width), lambda i: (0, 0)),
        ],
        out_specs=pl.BlockSpec((1, rows, width), lambda i: (i, 0, 0)),
        out_shape=jax.ShapeDtypeStruct(blocks.shape, jnp.bfloat16),
        cost_estimate=pl.CostEstimate(flops=40 * n * rows * width, bytes_accessed=4 * n * rows * width, transcendentals=0),
        name="norm_rows",
    )(blocks, gain.reshape(1, width))


def attend_kernel(groups, head_dim, q_start, k_start, lens, q_ref, ka_ref, kb_ref, va_ref, vb_ref, c_ref):
    blk = pl.program_id(1)
    rows = q_ref.shape[0]
    keys = ka_ref.shape[1]
    q_all = jnp.concatenate([q_ref[:, g * head_dim:(g + 1) * head_dim] for g in range(groups)], axis=0)
    shape = (groups, rows, keys)
    q_pos = q_start[blk] + lax.broadcasted_iota(jnp.int32, shape, 1).reshape(groups * rows, keys)
    k_off = lax.broadcasted_iota(jnp.int32, (groups * rows, keys), 1)
    last = jnp.minimum(q_pos, lens[blk] - 1)

    def score(k_ref, start):
        s = lax.dot_general(q_all, k_ref[0], (((1,), (1,)), ((), ())), preferred_element_type=jnp.float32)
        return jnp.where(k_off + start <= last, s * (head_dim ** -0.5), -1e30)

    s_a = score(ka_ref, k_start[0])
    s_b = score(kb_ref, k_start[1])
    top = jnp.maximum(jnp.max(s_a, axis=-1, keepdims=True), jnp.max(s_b, axis=-1, keepdims=True))
    e_a = jnp.exp(s_a - top)
    e_b = jnp.exp(s_b - top)
    inv = 1.0 / (jnp.sum(e_a, axis=-1, keepdims=True) + jnp.sum(e_b, axis=-1, keepdims=True))
    ctx = jnp.dot((e_a * inv).astype(jnp.bfloat16), va_ref[0], preferred_element_type=jnp.float32)
    ctx += jnp.dot((e_b * inv).astype(jnp.bfloat16), vb_ref[0], preferred_element_type=jnp.float32)
    ctx = ctx.astype(jnp.bfloat16)
    for g in range(groups):
        c_ref[:, g * head_dim:(g + 1) * head_dim] = ctx[g * rows:(g + 1) * rows]


def attend(q_rot, kv_pair, parts, rows, q_start, k_start, lens, groups, head_dim):
    tokens, width = q_rot.shape
    n_blk = tokens // rows
    kv_heads = width // (groups * head_dim)
    keys = kv_pair[0].shape[1] // parts

    def kv_spec(half, first):
        def index(j, i, *_):
            return (i if parts == 2 else 0, half if parts == 2 else 0, first + j)
        return pl.BlockSpec((1, keys, head_dim), index)

    return pl.pallas_call(
        functools.partial(attend_kernel, groups, head_dim),
        grid_spec=pltpu.PrefetchScalarGridSpec(
            num_scalar_prefetch=3,
            grid=(kv_heads, n_blk),
            in_specs=[pl.BlockSpec((rows, groups * head_dim), lambda j, i, *_: (i, j)), kv_spec(0, 0), kv_spec(1, 0), kv_spec(0, kv_heads), kv_spec(1, kv_heads)],
            out_specs=pl.BlockSpec((rows, groups * head_dim), lambda j, i, *_: (i, j)),
        ),
        out_shape=jax.ShapeDtypeStruct(q_rot.shape, jnp.bfloat16),
        cost_estimate=pl.CostEstimate(flops=32 * tokens * width * keys, bytes_accessed=8 * tokens * width, transcendentals=0),
        name="attend",
    )(q_start, k_start, lens, q_rot, kv_pair[0], kv_pair[1], kv_pair[0], kv_pair[1])


def solution(mesh):
    n_dev = mesh.shape['tp']
    n_chip = n_dev // 2
    swap = [(d, d ^ 1) for d in range(n_dev)]

    def device_fn(hidden_in, lengths, attn_norm, w_query, w_key, w_value, w_out, mlp_norm, w_gate, w_up, w_down, final_norm):
        batch, seq_dev, d_model = hidden_in.shape
        heads, head_dim = w_query.shape[2], w_query.shape[3]
        kv_heads = w_key.shape[2]
        groups = heads // kv_heads
        n_stream = batch // n_chip
        quarter = n_dev // 2
        half_len = quarter * seq_dev
        me = lax.axis_index('tp')
        chip, side = me // 2, me % 2

        def project(hidden, weights, gain, q_pos):
            w_q, w_k, w_v = weights
            tokens = hidden.shape[0]
            cos_tab, sin_tab = rope_tables(q_pos, head_dim)
            normed = rms_norm(hidden, gain)
            k_proj = jnp.einsum('td,dhe->the', normed, w_k, preferred_element_type=jnp.float32)
            k_rot = rotate(k_proj, cos_tab, sin_tab).astype(jnp.bfloat16).reshape(tokens, -1)
            v_proj = jnp.einsum('td,dhe->the', normed, w_v, preferred_element_type=jnp.float32)
            v_proj = v_proj.astype(jnp.bfloat16).reshape(tokens, -1)
            q_proj = jnp.einsum('td,dhe->the', normed, w_q, preferred_element_type=jnp.float32)
            q_rot = rotate(q_proj, cos_tab, sin_tab).astype(jnp.bfloat16).reshape(tokens, -1)
            return q_rot, jnp.concatenate([k_rot, v_proj], axis=-1)

        def add_out(hidden, context, w_mat):
            w_mat = w_mat.reshape(heads * head_dim, d_model)
            attn_out = jnp.dot(context, w_mat, preferred_element_type=jnp.float32)
            return (hidden.astype(jnp.float32) + attn_out).astype(jnp.bfloat16)

        def mlp(gathered, layer, major):
            normed = norm_rows(gathered, mlp_norm[layer], major).reshape(-1, d_model)
            gate_proj = jnp.dot(normed, w_gate[layer], preferred_element_type=jnp.float32)
            up_proj = jnp.dot(normed, w_up[layer], preferred_element_type=jnp.float32)
            gated_act = (jax.nn.silu(gate_proj) * up_proj).astype(jnp.bfloat16)
            part_out = jnp.dot(gated_act, w_down[layer], preferred_element_type=jnp.float32)
            part_out = lax.reduce_precision(part_out, 8, 7)
            return lax.psum_scatter(part_out.reshape(n_dev, -1, d_model), 'tp', scatter_dimension=0, tiled=False)

        pos0 = jnp.tile(me * seq_dev + jnp.arange(seq_dev), n_chip)
        start0 = jnp.broadcast_to(me * seq_dev, (n_chip,)).astype(jnp.int32)
        pos1 = side * half_len + jnp.arange(half_len)
        start1 = (side * half_len + seq_dev * jnp.arange(quarter)).astype(jnp.int32)
        keys0 = (half_len * jnp.arange(2)).astype(jnp.int32)
        keys1 = jnp.stack([side * half_len, (1 - side) * half_len]).astype(jnp.int32)
        hid = hidden_in.reshape(n_chip, n_stream, seq_dev, d_model)
        lens = lengths.reshape(n_chip, n_stream)
        streams = range(n_stream)

        hidden = [hid[:, g].reshape(n_chip * seq_dev, d_model) for g in streams]
        weights = (w_query[0], w_key[0], w_value[0])
        qkv = [project(hidden[g], weights, attn_norm[0], pos0) for g in streams]
        wide = []
        for g in streams:
            q_rot, kv_own = qkv[g]
            kv_all = lax.all_gather(kv_own.reshape(n_chip, seq_dev, -1), 'tp', axis=1, tiled=True)
            context = attend(q_rot, (kv_all, kv_all), 2, seq_dev, start0, keys0, lens[:, g], groups, head_dim)
            hidden[g] = add_out(hidden[g], context, w_out[0])
            wide.append(lax.all_gather(hidden[g], 'tp', axis=0, tiled=True).reshape(n_dev * n_chip, seq_dev, d_model))

        total = [mlp(wide[g], 0, n_chip) for g in streams]
        before = None
        later = lax.optimization_barrier((w_query, w_key, w_value, w_out, wide[-1]))
        weights = tuple(w[1] for w in later[:4])
        for g in streams:
            if before is not None:
                total[g] = lax.optimization_barrier((total[g], before))[0]
            mine = lax.dynamic_slice(wide[g].reshape(2, quarter, n_chip, seq_dev, d_model), (side, 0, chip, 0, 0), (1, quarter, 1, seq_dev, d_model))
            hidden[g] = (mine.reshape(half_len, d_model).astype(jnp.float32) + total[g]).astype(jnp.bfloat16)
            q_rot, kv_own = project(hidden[g], weights[:3], attn_norm[1], pos1)
            kv_own = kv_own[None]
            kv_far = lax.ppermute(kv_own, 'tp', swap)
            len_g = jnp.broadcast_to(lax.dynamic_slice(lens[:, g], (chip,), (1,)), (quarter,))
            context = attend(q_rot, (kv_own, kv_far), 1, seq_dev, start1, keys1, len_g, groups, head_dim)
            hidden[g] = add_out(hidden[g], context, weights[3])
            before = hidden[g]
            wide[g] = lax.all_gather(hidden[g], 'tp', axis=0, tiled=True).reshape(n_dev * n_chip, seq_dev, d_model)

        total = [mlp(wide[g], 1, n_dev) for g in streams]
        outs = []
        for g in streams:
            mine = lax.dynamic_slice(wide[g].reshape(n_chip, n_dev, seq_dev, d_model), (0, me, 0, 0), (n_chip, 1, seq_dev, d_model))
            last = (mine.reshape(n_chip, seq_dev, d_model).astype(jnp.float32) + total[g].reshape(n_chip, seq_dev, d_model)).astype(jnp.bfloat16)
            outs.append(rms_norm(last, final_norm))
        return jnp.stack(outs, axis=1).reshape(batch, seq_dev, d_model)

    seq_part = P(None, 'tp', None)
    in_specs = (seq_part, P(), P(), P(), P(), P(), P(), P(), P(None, None, 'tp'), P(None, None, 'tp'), P(None, 'tp', None), P())
    return jax.shard_map(device_fn, mesh=mesh, in_specs=in_specs, out_specs=seq_part, check_vma=False)
```

```python
import functools

import jax
import jax.numpy as jnp
from jax import lax
from jax.experimental import pallas as pl
from jax.experimental.pallas import tpu as pltpu
from jax.sharding import PartitionSpec as P

NORM_EPS = 1e-5
ROPE_BASE = 500000.0


def rms_norm(hidden, gain):
    h_wide = hidden.astype(jnp.float32)
    inv_rms = lax.rsqrt(jnp.mean(h_wide * h_wide, axis=-1, keepdims=True) + NORM_EPS)
    return (h_wide * inv_rms * gain.astype(jnp.float32)).astype(jnp.bfloat16)


def rope_tables(positions, head_dim):
    half_dim = head_dim // 2
    inv_freq = ROPE_BASE ** (-2.0 * jnp.arange(half_dim).astype(jnp.float32) / head_dim)
    angles = positions.astype(jnp.float32)[:, None, None] * inv_freq[None, None, :]
    return jnp.cos(angles), jnp.sin(angles)


def rotate(proj, cos_tab, sin_tab):
    half_dim = proj.shape[-1] // 2
    first = proj[..., :half_dim]
    second = proj[..., half_dim:]
    return jnp.concatenate([first * cos_tab - second * sin_tab, second * cos_tab + first * sin_tab], axis=-1)


def norm_kernel(source, side, near_ref, far_ref, gain_ref, z_ref):
    i, half = pl.program_id(0), pl.num_programs(0) // 2
    owner = jnp.where(i < half, 1 - side[0], side[0])
    is_near = source(owner, lax.rem(i, half))[0] == side[0]
    pl.when(is_near)(lambda: norm_block(near_ref, gain_ref, z_ref))
    pl.when(jnp.logical_not(is_near))(lambda: norm_block(far_ref, gain_ref, z_ref))


def norm_block(h_ref, gain_ref, z_ref):
    rows, width = h_ref.shape[1:]
    step, span = 16, min(512, width)

    def part(i, carry):
        at = pl.ds(pl.multiple_of(i * step, step), step)
        acc = jnp.zeros((step, span), jnp.float32)
        for c in range(0, width, span):
            wide = h_ref[0, at, c:c + span].astype(jnp.float32)
            acc += wide * wide
        inv_rms = lax.rsqrt(jnp.sum(acc, axis=-1, keepdims=True) * (1.0 / width) + NORM_EPS)
        for c in range(0, width, span):
            wide = h_ref[0, at, c:c + span].astype(jnp.float32)
            z_ref[0, at, c:c + span] = (wide * inv_rms * gain_ref[:, c:c + span]).astype(z_ref.dtype)
        return carry

    lax.fori_loop(0, rows // step, part, 0)


def norm_rows(near, far, gain, side, source):
    half, rows, width = near.shape

    def index(is_near):
        def of(i, side_ref):
            owner = jnp.where(i < half, 1 - side_ref[0], side_ref[0])
            from_side, block = source(owner, i % half)
            if source.alternates:
                return (block, 0, 0)
            used = (from_side == side_ref[0]) == is_near
            return (jnp.where(used, block, 0), 0, 0)
        return of

    return pl.pallas_call(
        functools.partial(norm_kernel, source),
        grid_spec=pltpu.PrefetchScalarGridSpec(
            num_scalar_prefetch=1,
            grid=(2 * half,),
            in_specs=[
                pl.BlockSpec((1, rows, width), index(True)),
                pl.BlockSpec((1, rows, width), index(False)),
                pl.BlockSpec((1, width), lambda i, _: (0, 0)),
            ],
            out_specs=pl.BlockSpec((1, rows, width), lambda i, _: (i, 0, 0)),
        ),
        out_shape=jax.ShapeDtypeStruct((2 * half, rows, width), jnp.bfloat16),
        cost_estimate=pl.CostEstimate(flops=80 * half * rows * width, bytes_accessed=8 * half * rows * width, transcendentals=0),
        name="norm_rows",
    )(side.reshape(1), near, far, gain.astype(jnp.float32).reshape(1, width))


def add_out_kernel(c_ref, w_ref, h_ref, o_ref):
    out = jnp.dot(c_ref[...], w_ref[0], preferred_element_type=jnp.float32)
    o_ref[...] = (h_ref[...].astype(jnp.float32) + out).astype(o_ref.dtype)


def add_out(hidden, context, w_all, layer):
    tokens, depth = context.shape
    width = hidden.shape[1]
    span = min(512, width)
    return pl.pallas_call(
        add_out_kernel,
        grid=(width // span,),
        in_specs=[
            pl.BlockSpec((tokens, depth), lambda j: (0, 0)),
            pl.BlockSpec((1, depth, span), lambda j: (layer, 0, j)),
            pl.BlockSpec((tokens, span), lambda j: (0, j)),
        ],
        out_specs=pl.BlockSpec((tokens, span), lambda j: (0, j)),
        out_shape=jax.ShapeDtypeStruct(hidden.shape, jnp.bfloat16),
        cost_estimate=pl.CostEstimate(flops=2 * tokens * depth * width, bytes_accessed=2 * depth * width, transcendentals=0),
        name="add_out",
    )(context, w_all, hidden)


def attend_kernel(groups, head_dim, q_start, k_start, lens, q_ref, ka_ref, kb_ref, va_ref, vb_ref, c_ref):
    blk = pl.program_id(1)
    rows = q_ref.shape[0]
    keys = ka_ref.shape[1]
    q_all = jnp.concatenate([q_ref[:, g * head_dim:(g + 1) * head_dim] for g in range(groups)], axis=0)
    shape = (groups, rows, keys)
    q_pos = q_start[blk] + lax.broadcasted_iota(jnp.int32, shape, 1).reshape(groups * rows, keys)
    k_off = lax.broadcasted_iota(jnp.int32, (groups * rows, keys), 1)
    last = jnp.minimum(q_pos, lens[blk] - 1)

    def score(k_ref, start):
        s = lax.dot_general(q_all, k_ref[0], (((1,), (1,)), ((), ())), preferred_element_type=jnp.float32)
        return jnp.where(k_off + start <= last, s * (head_dim ** -0.5), -1e30)

    s_a = score(ka_ref, k_start[0])
    s_b = score(kb_ref, k_start[1])
    top = jnp.maximum(jnp.max(s_a, axis=-1, keepdims=True), jnp.max(s_b, axis=-1, keepdims=True))
    e_a = jnp.exp(s_a - top)
    e_b = jnp.exp(s_b - top)
    inv = 1.0 / (jnp.sum(e_a, axis=-1, keepdims=True) + jnp.sum(e_b, axis=-1, keepdims=True))
    ctx = jnp.dot((e_a * inv).astype(jnp.bfloat16), va_ref[0], preferred_element_type=jnp.float32)
    ctx += jnp.dot((e_b * inv).astype(jnp.bfloat16), vb_ref[0], preferred_element_type=jnp.float32)
    ctx = ctx.astype(jnp.bfloat16)
    for g in range(groups):
        c_ref[:, g * head_dim:(g + 1) * head_dim] = ctx[g * rows:(g + 1) * rows]


def attend(q_rot, kv_pair, parts, rows, q_start, k_start, lens, groups, head_dim):
    tokens, width = q_rot.shape
    n_blk = tokens // rows
    kv_heads = width // (groups * head_dim)
    keys = kv_pair[0].shape[1] // parts

    def kv_spec(half, first):
        def index(j, i, *_):
            return (i if parts == 2 else 0, half if parts == 2 else 0, first + j)
        return pl.BlockSpec((1, keys, head_dim), index)

    return pl.pallas_call(
        functools.partial(attend_kernel, groups, head_dim),
        grid_spec=pltpu.PrefetchScalarGridSpec(
            num_scalar_prefetch=3,
            grid=(kv_heads, n_blk),
            in_specs=[pl.BlockSpec((rows, groups * head_dim), lambda j, i, *_: (i, j)), kv_spec(0, 0), kv_spec(1, 0), kv_spec(0, kv_heads), kv_spec(1, kv_heads)],
            out_specs=pl.BlockSpec((rows, groups * head_dim), lambda j, i, *_: (i, j)),
        ),
        out_shape=jax.ShapeDtypeStruct(q_rot.shape, jnp.bfloat16),
        cost_estimate=pl.CostEstimate(flops=32 * tokens * width * keys, bytes_accessed=8 * tokens * width, transcendentals=0),
        name="attend",
    )(q_start, k_start, lens, q_rot, kv_pair[0], kv_pair[1], kv_pair[0], kv_pair[1])


def solution(mesh):
    n_dev = mesh.shape['tp']
    n_chip = n_dev // 2
    swap = [(d, d ^ 1) for d in range(n_dev)]
    same_side = [list(range(s, n_dev, 2)) for s in range(2)]

    def device_fn(hidden_in, lengths, attn_norm, w_query, w_key, w_value, w_out, mlp_norm, w_gate, w_up, w_down, final_norm):
        batch, seq_dev, d_model = hidden_in.shape
        heads, head_dim = w_query.shape[2], w_query.shape[3]
        kv_heads = w_key.shape[2]
        groups = heads // kv_heads
        n_stream = batch // n_chip
        quarter = n_dev // 2
        half_len = quarter * seq_dev
        me = lax.axis_index('tp')
        chip, side = me // 2, me % 2

        def project(hidden, weights, gain, q_pos):
            w_q, w_k, w_v = weights
            tokens = hidden.shape[0]
            cos_tab, sin_tab = (t.reshape(-1, seq_dev, 1, head_dim // 2) for t in rope_tables(q_pos, head_dim))
            normed = rms_norm(hidden.reshape(-1, seq_dev, d_model), gain)
            k_proj = jnp.einsum('bsd,dhe->bshe', normed, w_k, preferred_element_type=jnp.float32)
            k_rot = rotate(k_proj, cos_tab, sin_tab).astype(jnp.bfloat16).reshape(tokens, -1)
            v_proj = jnp.einsum('bsd,dhe->bshe', normed, w_v, preferred_element_type=jnp.float32)
            v_proj = v_proj.astype(jnp.bfloat16).reshape(tokens, -1)
            q_proj = jnp.einsum('bsd,dhe->bshe', normed, w_q, preferred_element_type=jnp.float32)
            q_rot = rotate(q_proj, cos_tab, sin_tab).astype(jnp.bfloat16).reshape(tokens, -1)
            return q_rot, jnp.concatenate([k_rot, v_proj], axis=-1)

        def spread(hidden):
            return lax.all_gather(hidden, 'tp', axis=0, tiled=True, axis_index_groups=same_side)

        def mlp_all(near, layer, source):
            pairs, wides, acts = [], [], []

            def down(g):
                act = acts[g]
                far = act.shape[0] // 2
                far_out = jnp.dot(act[:far], w_down[layer], preferred_element_type=jnp.float32).astype(jnp.bfloat16)
                from_core = lax.ppermute(far_out, 'tp', swap)
                own_out = jnp.dot(act[far:], w_down[layer], preferred_element_type=jnp.float32)
                pairs.append(lax.reduce_precision(own_out, 8, 7) + from_core.astype(jnp.float32))

            for g in streams:
                now = near[g]
                if g > 0:
                    now, acts[-1] = lax.optimization_barrier((now, acts[-1]))
                    down(g - 1)
                wides.append(tuple(w.reshape(-1, seq_dev, d_model) for w in (now, lax.ppermute(now, 'tp', swap))))
                normed = norm_rows(*wides[-1], mlp_norm[layer], side, source).reshape(-1, d_model)
                gate_proj = jnp.dot(normed, w_gate[layer], preferred_element_type=jnp.float32)
                up_proj = jnp.dot(normed, w_up[layer], preferred_element_type=jnp.float32)
                acts.append((jax.nn.silu(gate_proj) * up_proj).astype(jnp.bfloat16))
            down(n_stream - 1)
            return pairs, wides

        def scatter(pair):
            return lax.psum_scatter(pair.reshape(n_chip, -1, d_model), 'tp', scatter_dimension=0, axis_index_groups=same_side, tiled=False)

        pos0 = jnp.tile(me * seq_dev + jnp.arange(seq_dev), n_chip)
        start0 = jnp.broadcast_to(me * seq_dev, (n_chip,)).astype(jnp.int32)
        pos1 = side * half_len + jnp.arange(half_len)
        start1 = (side * half_len + seq_dev * jnp.arange(quarter)).astype(jnp.int32)
        keys0 = (half_len * jnp.arange(2)).astype(jnp.int32)
        keys1 = jnp.stack([side * half_len, (1 - side) * half_len]).astype(jnp.int32)
        w_out_mat = w_out.reshape(-1, heads * head_dim, d_model)
        hid = hidden_in.reshape(n_chip, n_stream, seq_dev, d_model)
        lens = lengths.reshape(n_chip, n_stream)
        streams = range(n_stream)

        hidden = [hid[:, g].reshape(n_chip * seq_dev, d_model) for g in streams]
        weights = (w_query[0], w_key[0], w_value[0])
        qkv = [project(hidden[g], weights, attn_norm[0], pos0) for g in streams]
        near = []
        held = lax.optimization_barrier((qkv[0][0],) + tuple(kv for _, kv in qkv[1:]))
        qkv = [(held[0], qkv[0][1])] + [(q, kv) for (q, _), kv in zip(qkv[1:], held[1:])]
        for g in streams:
            q_rot, kv_own = qkv[g]
            kv_all = lax.all_gather(kv_own.reshape(n_chip, seq_dev, -1), 'tp', axis=1, tiled=True)
            context = attend(q_rot, (kv_all, kv_all), 2, seq_dev, start0, keys0, lens[:, g], groups, head_dim)
            hidden[g] = add_out(hidden[g], context, w_out_mat, 0)
            near.append(spread(hidden[g]))

        def source0(s, i):
            from_dev = s * quarter + i % quarter
            return from_dev % 2, (from_dev // 2) * n_chip + i // quarter

        def source1(s, i):
            shard = 2 * (i // n_chip) + s
            return shard // quarter, (i % n_chip) * quarter + shard % quarter

        source0.alternates, source1.alternates = True, False
        pairs, wide = mlp_all(near, 0, source0)
        late_one, pairs[-1] = lax.optimization_barrier((jnp.int32(1), pairs[-1]))
        weights = tuple(lax.dynamic_index_in_dim(w, late_one, 0, keepdims=False) for w in (w_query, w_key, w_value))
        total = [scatter(p) for p in pairs]
        near1 = []
        for g in streams:
            if g > 0:
                total[g], hidden[g - 1] = lax.optimization_barrier((total[g], hidden[g - 1]))
                near1.append(spread(hidden[g - 1]))
            from_near, from_far = (lax.dynamic_slice(w.reshape(n_chip, n_chip, seq_dev, d_model), (side * (quarter // 2), chip, 0, 0), (quarter // 2, 1, seq_dev, d_model)) for w in wide[g])
            mine = jnp.where(side == 0, jnp.concatenate([from_near, from_far], axis=1), jnp.concatenate([from_far, from_near], axis=1))
            hidden[g] = (mine.reshape(half_len, d_model).astype(jnp.float32) + total[g]).astype(jnp.bfloat16)
            q_rot, kv_own = project(hidden[g], weights, attn_norm[1], pos1)
            kv_own = kv_own[None]
            kv_far = lax.ppermute(kv_own, 'tp', swap)
            len_g = jnp.broadcast_to(lax.dynamic_slice(lens[:, g], (chip,), (1,)), (quarter,))
            context = attend(q_rot, (kv_own, kv_far), 1, seq_dev, start1, keys1, len_g, groups, head_dim)
            hidden[g] = add_out(hidden[g], context, w_out_mat, 1)
        near1[0], hidden[-1] = lax.optimization_barrier((near1[0], hidden[-1]))
        near1.append(spread(hidden[-1]))

        pairs, wide = mlp_all(near1, 1, source1)
        total = [scatter(p) for p in pairs]
        outs = []
        for g in streams:
            from_near, from_far = (lax.dynamic_slice(w.reshape(n_chip, quarter, seq_dev, d_model), (0, me % quarter, 0, 0), (n_chip, 1, seq_dev, d_model)) for w in wide[g])
            mine = jnp.where(me // quarter == side, from_near, from_far)
            last = (mine.reshape(n_chip, seq_dev, d_model).astype(jnp.float32) + total[g].reshape(n_chip, seq_dev, d_model)).astype(jnp.bfloat16)
            outs.append(rms_norm(last, final_norm))
        return jnp.stack(outs, axis=1).reshape(batch, seq_dev, d_model)

    seq_part = P(None, 'tp', None)
    in_specs = (seq_part, P(), P(), P(), P(), P(), P(), P(), P(None, None, 'tp'), P(None, None, 'tp'), P(None, 'tp', None), P())
    return jax.shard_map(device_fn, mesh=mesh, in_specs=in_specs, out_specs=seq_part, check_vma=False)
```
